256 devices in a mesh: expert: 32 (over x, z_lo, y), dp: 8 (over z_hi, core).
Axes of the slice: x: 4, y: 4, z: 8 (z_hi: 4, z_lo: 2; z = z_hi * 2 + z_lo), core: 2. Of those that a mesh axis runs over, the one named last changes fastest.
Arguments:
- tokens: bfloat16 [32768, 1440], P(('expert', 'dp')), may hold values from -6 to 6
- cotangent: bfloat16 [32768, 1440], P(('expert', 'dp')), may hold values from -0.3984375 to 0.3984375
- expert_ids: int32 [32768, 4], P(('expert', 'dp')), may hold values from 0 to 31, all different within a row; in each aligned block of 128 rows (0 to 127, 128 to 255, ...) at most 24 rows name the same one
- gate_weights: float32 [32768, 4], P(('expert', 'dp')), may hold values from 0.05 to 1
- w_gate: bfloat16 [32, 1440, 1440], P('expert', 'dp'), may hold values from -0.15625 to 0.15625
- w_up: bfloat16 [32, 1440, 1440], P('expert', 'dp'), may hold values from -0.15625 to 0.15625
- w_down: bfloat16 [32, 1440, 1440], P('expert', 'dp'), may hold values from -0.15625 to 0.15625
Outputs:
- mixed: bfloat16 [32768, 1440], P(('expert', 'dp'))
- grad_gate: bfloat16 [32, 1440, 1440], P('expert', 'dp')
- grad_up: bfloat16 [32, 1440, 1440], P('expert', 'dp')
- grad_down: bfloat16 [32, 1440, 1440], P('expert', 'dp')
The draws below stay inside these ranges and needn't reach their ends.
Inputs may be any that keep to these rules, and one draw needn't show every extreme that they name: `expert_ids`: each row names 4 different experts. Within the rows of one device no expert is named more than 24 times, a bound that some block reaches.
All inputs are finite; a program needn't handle non-finite values.
Results may differ from the reference program's by a relative error of at most 0.013.
Values may be sent and summed in bfloat16 or wider, within the bound.
No kernel may reach another device: no remote copies, remote signals or barrier semaphores. Data moves between devices by JAX's collectives and lax.ppermute only.
A program may use at most 128 MiB of HBM per device.

```python
import math
import jax
import jax.numpy as jnp
import numpy as np
from jax import lax

D = 1440
FH = 1440
TOPK = 4
TOK_DEV = 128
CAP = 512
EXPERTS = 32
SLOT = 24
TOKENS = 32768
N_EXPERT = 32
N_DP = 8


def shard_levels(key, dims, pieces, smallest, high):
    level = 1.0
    for dim, shards_of in pieces:
        draws = jax.random.uniform(jax.random.fold_in(jax.random.fold_in(key, 6), dim), (shards_of,), jnp.float32, smallest / len(pieces), high / len(pieces))
        level = level * jnp.repeat(jnp.exp(draws), dims[dim] // shards_of).reshape((-1,) + (1,) * (len(dims) - 1 - dim))
    return level


def routed_block(stream_key, own, number, rows, number_of, top, reach, skew):
    ranking = jax.random.permutation(stream_key, number_of)
    packed, usual = shares(number_of, rows * top, reach, skew, True), shares(number_of, rows * top, reach, skew, False)
    places = jnp.arange(number_of)

    def named(sizes, offset_by):
        used = int((sizes > 0).sum())
        fixed = max(1, used // 4)
        shifted = fixed + (places - fixed + offset_by * (used - fixed)) % max(1, number_of - fixed)
        return jnp.zeros((number_of,), jnp.int32).at[ranking[jnp.where(places < fixed, places, shifted)]].set(jnp.asarray(sizes, jnp.int32))

    sizes = jnp.where(number % 4 == 0, named(packed, number // 4), named(usual, number - number // 4 - 1))
    mixed = jax.random.permutation(jax.random.fold_in(own, 3), number_of)
    giver, receiver = mixed[0:number_of // 2 * 2:2], mixed[1:number_of // 2 * 2:2]
    margin = jnp.minimum(sizes[giver] - 1, reach - sizes[receiver]) // 2
    margin = jnp.where((giver == ranking[0]) | (receiver == ranking[0]) | (sizes[receiver] == 0), 0, jnp.maximum(margin, 0))
    shifted = jax.random.randint(jax.random.fold_in(own, 4), (number_of // 2,), 0, 1 << 20) % (margin + 1)
    sizes = sizes.at[giver].add(-shifted).at[receiver].add(shifted)
    items = jnp.searchsorted(jnp.cumsum(sizes), jnp.arange(rows * top), side="right").astype(jnp.int32)
    listing = items.reshape(top, rows).T
    listing = listing[jax.random.permutation(jax.random.fold_in(own, 1), rows)]
    offset_by = jax.random.randint(jax.random.fold_in(own, 2), (rows, 1), 0, top)
    return jnp.take_along_axis(listing, (jnp.arange(top)[None, :] + offset_by) % top, axis=1)


def shares(count, total, bound, skew, full):
    weights = [(1 << 20) // math.isqrt(rank ** skew) + 1 for rank in range(1, count + 1)]
    largest = bound if full else min(bound, max(-(-total // count), total * weights[0] // sum(weights)))
    least = 1 if total - largest >= count - 1 else 0
    holding, rest = [largest] + [least] * (count - 1), total - largest - least * (count - 1)
    while rest > 0:
        candidates = [i for i in range(1, count) if holding[i] < largest] or [i for i in range(1, count) if holding[i] < bound]
        pool, left = sum([weights[i] for i in candidates]), rest
        for i in candidates:
            extra = min(bound - holding[i], max(1, left * weights[i] // pool), rest)
            holding[i] = holding[i] + extra
            rest = rest - extra
    return np.array(holding)


def centred(own_key, extent, scale, reach, split=(), kind=jnp.bfloat16):
    entries = scale * jax.random.normal(own_key, extent, jnp.float32)
    if split:
        entries = entries * shard_levels(own_key, extent, split, -0.22, 0.18)
    return jnp.clip(entries, -reach, reach).astype(kind)


def setup_inputs(seed: int = 0) -> dict:
    splits = jax.random.split(jax.random.key(seed), 8)
    tokens = centred(splits[0], (TOKENS, D), 1.0, 6.0, ((0, 256),))
    cotangent = centred(splits[1], (TOKENS, D), 0.05, 0.3984375, ((0, 256),))
    expert_ids_keys = jax.random.split(jax.random.fold_in(splits[2], 1), TOKENS // TOK_DEV)
    expert_ids_turns = jax.random.permutation(jax.random.fold_in(splits[2], 3), TOKENS // TOK_DEV)
    expert_ids = jax.vmap(lambda own, number: routed_block(jax.random.fold_in(splits[2], 2), own, number, TOK_DEV, EXPERTS, TOPK, SLOT, 2))(expert_ids_keys, expert_ids_turns).reshape((TOKENS, TOPK))
    gate_weights = jnp.clip(jnp.exp(math.log(1.0) - 2.9957323 * jax.random.uniform(splits[3], (TOKENS, TOPK), jnp.float32) ** shard_levels(splits[3], (TOKENS, TOPK), ((0, 256),), -0.2, 0.2)), 0.05, 1.0)
    w_gate = centred(splits[4], (EXPERTS, D, FH), D ** -0.5, 0.15625, ((0, 32), (1, 8)))
    w_up = centred(splits[5], (EXPERTS, D, FH), D ** -0.5, 0.15625, ((0, 32), (1, 8)))
    w_down = centred(splits[6], (EXPERTS, D, FH), FH ** -0.5, 0.15625, ((0, 32), (1, 8)))
    return dict(tokens=tokens, cotangent=cotangent, expert_ids=expert_ids, gate_weights=gate_weights, w_gate=w_gate, w_up=w_up, w_down=w_down)


SWISH_SLOPE = 1.702


def expert_pass(packed_x, packed_g, gate_mat, up_mat, down_mat):
    pre_gate = jnp.dot(packed_x, gate_mat, preferred_element_type=jnp.float32)
    pre_up = jnp.dot(packed_x, up_mat, preferred_element_type=jnp.float32)
    sigmoid_part = jax.nn.sigmoid(SWISH_SLOPE * pre_gate)
    value = pre_gate * sigmoid_part
    slope_term = sigmoid_part + SWISH_SLOPE * pre_gate * sigmoid_part * (1.0 - sigmoid_part)
    hidden = (value * (pre_up + 1.0)).astype(jnp.bfloat16)
    expert_out = jnp.dot(hidden, down_mat.T, preferred_element_type=jnp.float32).astype(jnp.bfloat16)
    d_hidden = jnp.dot(packed_g, down_mat, preferred_element_type=jnp.float32)
    grad_down = jnp.dot(packed_g.T, hidden, preferred_element_type=jnp.float32)
    d_gate = (d_hidden * (pre_up + 1.0) * slope_term).astype(jnp.bfloat16)
    d_up = (d_hidden * value).astype(jnp.bfloat16)
    grad_gate = jnp.dot(packed_x.T, d_gate, preferred_element_type=jnp.float32)
    grad_up = jnp.dot(packed_x.T, d_up, preferred_element_type=jnp.float32)
    return expert_out, jnp.stack([grad_gate, grad_up, grad_down]).astype(jnp.bfloat16)


def reference(tokens, cotangent, expert_ids, gate_weights, w_gate, w_up, w_down):
    assigns = TOK_DEV * TOPK
    expert_table = jnp.arange(EXPERTS, dtype=jnp.int32)

    def rank_block(block):
        onehot = (block[:, None] == expert_table[None, :]).astype(jnp.int32)
        local_rank = jnp.sum((jnp.cumsum(onehot, axis=0) - onehot) * onehot, axis=1)
        return local_rank, jnp.sum(onehot, axis=0)

    local_rank, block_counts = lax.map(rank_block, expert_ids.reshape(N_EXPERT * N_DP, assigns))
    local_rank = local_rank.reshape(N_EXPERT, N_DP, assigns)
    block_counts = block_counts.reshape(N_EXPERT, N_DP, EXPERTS)
    offsets = jnp.cumsum(block_counts, axis=0) - block_counts
    group_ids = expert_ids.reshape(N_EXPERT, N_DP, assigns)
    position = jnp.take_along_axis(offsets, group_ids, axis=2) + local_rank
    target = jnp.where(position < CAP, position, CAP).astype(jnp.int32)
    gates = gate_weights.reshape(N_EXPERT, N_DP, assigns)
    token_rows = tokens.reshape(N_EXPERT, N_DP, TOK_DEV, D)
    cot_rows = cotangent.reshape(N_EXPERT, N_DP, TOK_DEV, D)
    inputs = (jnp.swapaxes(group_ids, 0, 1), jnp.swapaxes(target, 0, 1), jnp.swapaxes(gates, 0, 1),
              jnp.swapaxes(token_rows, 0, 1), jnp.swapaxes(cot_rows, 0, 1))

    def run_expert(item):
        return expert_pass(item[0], item[1], item[2], item[3], item[4])

    def per_group(totals, group):
        ids_here, target_here, gates_here, tokens_here, cot_here = group
        token_copies = jnp.repeat(tokens_here, TOPK, axis=1)
        gated = (gates_here[:, :, None] * jnp.repeat(cot_here, TOPK, axis=1).astype(jnp.float32)).astype(jnp.bfloat16)
        packed_x = jnp.zeros((EXPERTS, CAP, D), jnp.bfloat16).at[ids_here, target_here].set(token_copies, mode="drop")
        packed_g = jnp.zeros((EXPERTS, CAP, D), jnp.bfloat16).at[ids_here, target_here].set(gated, mode="drop")
        outputs, group_grads = lax.map(run_expert, (packed_x, packed_g, w_gate, w_up, w_down))
        group_grads = lax.optimization_barrier(group_grads)
        totals = totals + group_grads.astype(jnp.float32)
        kept = (target_here < CAP).astype(jnp.float32)
        fetched = outputs[ids_here, jnp.minimum(target_here, CAP - 1)]
        weighted = (gates_here * kept)[:, :, None] * fetched.astype(jnp.float32)
        mixed_group = jnp.sum(weighted.reshape(N_EXPERT, TOK_DEV, TOPK, D), axis=2).astype(jnp.bfloat16)
        return totals, mixed_group

    totals = jnp.zeros((EXPERTS, 3, D, FH), jnp.float32)
    totals, mixed_all = lax.scan(per_group, totals, inputs)
    mixed = jnp.swapaxes(mixed_all, 0, 1).reshape(TOKENS, D)
    grads = totals.astype(jnp.bfloat16)
    return (mixed, grads[:, 0], grads[:, 1], grads[:, 2])
```

```python
import jax
import jax.numpy as jnp
from jax import lax
from jax.experimental import pallas as pl
from jax.experimental.pallas import tpu as pltpu
from jax.sharding import PartitionSpec as P


D = 1440
FH = 1440
CHUNK = 180
WIDE = 192
PADDED = 8 * WIDE
TOP = 4
TOK = 128
CAP = 512
SLOT = 24
PEERS = 16
ROWS = PEERS * 2 * SLOT
SWISH_SLOPE = 1.702
AXES = ("expert", "dp")
F32 = jnp.float32
BF16 = jnp.bfloat16


def device(e, d):
    return e * 8 + d


def zring(step):
    return [
        (device(e, z * 2 + c), device(e, ((z + step) % 4) * 2 + c))
        for e in range(32)
        for z in range(4)
        for c in range(2)
    ]


UP = zring(1)
DOWN = zring(-1)
CORES = [(device(e, d), device(e, d ^ 1)) for e in range(32) for d in range(8)]
PAIRS = [(device(e, d), device(e ^ 4, d)) for e in range(32) for d in range(8)]
PLANES = [[x * 8 + zl * 4 + y for x in range(4) for y in range(4)] for zl in range(2)]


def send(value, perm):
    return lax.ppermute(value, AXES, perm)


def iota(shape, dim):
    return lax.broadcasted_iota(jnp.int32, shape, dim)


def spread(shape, wide_dim):
    narrow = iota(shape, 1 - wide_dim)
    wide = iota(shape, wide_dim)
    chunk = wide // WIDE
    within = wide - chunk * WIDE
    return ((within < CHUNK) & (narrow == chunk * CHUNK + within)).astype(F32).astype(BF16)


def expert_of(q, zl):
    peer = q // (2 * SLOT)
    return (peer // 4) * 8 + zl * 4 + (peer - (peer // 4) * 4)


def slots_kernel(zl_ref, own_x, other_x, own_c, other_c, own_meta, other_meta, out):
    zl = zl_ref[0]
    grow = spread((D, PADDED), 1)
    used = jnp.zeros((1, PADDED), F32) + (iota((1, PADDED), 1) == CHUNK).astype(F32)
    x = jnp.concatenate([own_x[...], other_x[...]], axis=0)
    c = jnp.concatenate([own_c[...], other_c[...]], axis=0)
    xe = (jnp.dot(x, grow, preferred_element_type=F32) + used).astype(BF16)
    ce = jnp.dot(c, grow, preferred_element_type=F32).astype(BF16)
    q = iota((ROWS, TOK), 0)
    expert = expert_of(q, zl)
    inner = q - (q // (2 * SLOT)) * (2 * SLOT)
    block = inner // SLOT
    rank_of_slot = (inner - block * SLOT).astype(F32)
    earlier = (iota((TOK, TOK), 0) < iota((TOK, TOK), 1)).astype(F32).astype(BF16)
    masks = []
    gate = jnp.zeros((ROWS, 1), F32)
    for b, meta in enumerate((own_meta, other_meta)):
        ids = meta[0:TOP, :].astype(jnp.int32)
        named = jnp.zeros((ROWS, TOK), F32)
        weight = jnp.zeros((ROWS, TOK), F32)
        for k in range(TOP):
            hit = ids[k : k + 1, :] == expert
            named = jnp.where(hit, 1.0, named)
            weight = jnp.where(hit, meta[TOP + k : TOP + k + 1, :], weight)
        rank = jnp.dot(named.astype(BF16), earlier, preferred_element_type=F32)
        mask = (named > 0.5) & (rank == rank_of_slot) & (block == b)
        masks.append(mask.astype(F32).astype(BF16))
        gate = gate + jnp.sum(jnp.where(mask, weight, 0.0), axis=1, keepdims=True)
    m = jnp.concatenate(masks, axis=1)
    sx = jnp.dot(m, xe, preferred_element_type=F32).astype(BF16)
    sc = (jnp.dot(m, ce, preferred_element_type=F32) * gate).astype(BF16)
    out[:, 0 : 2 * SLOT, :] = sx.reshape(PEERS, 2 * SLOT, PADDED)
    out[:, 2 * SLOT : 4 * SLOT, :] = sc.reshape(PEERS, 2 * SLOT, PADDED)


def source_of(q, zl):
    peer = q // (2 * SLOT)
    inner = q - peer * (2 * SLOT)
    block = inner // SLOT
    plane = jnp.where(block == 0, zl, 1 - zl)
    return (peer // 4) * 8 + plane * 4 + (peer - (peer // 4) * 4), inner - block * SLOT


def pack_kernel(zl_ref, recv, px, pg, pt):
    zl = zl_ref[0]
    x = recv[:, 0 : 2 * SLOT, :].reshape(ROWS, PADDED)
    g = recv[:, 2 * SLOT : 4 * SLOT, :].reshape(ROWS, PADDED)
    flags = x[:, 128:256]
    lane = CHUNK - 128
    source_row, rank_row = source_of(iota((ROWS, ROWS), 1), zl)
    source_col, rank_col = source_of(iota((ROWS, ROWS), 0), zl)
    before = (source_col < source_row).astype(F32).astype(BF16)
    same = (iota((ROWS, ROWS), 0) == iota((ROWS, ROWS), 1)).astype(F32).astype(BF16)
    contract = (((0,), (0,)), ((), ()))
    start_row = lax.dot_general(flags, before, contract, preferred_element_type=F32)
    used_row = lax.dot_general(flags, same, contract, preferred_element_type=F32)
    start_row = start_row[lane : lane + 1, :].astype(jnp.int32) + rank_row[0:1, :]
    place_row = jnp.where(used_row[lane : lane + 1, :] > 0.5, start_row, CAP)
    p = (iota((CAP, ROWS), 0) == place_row).astype(F32).astype(BF16)
    px[...] = jnp.dot(p, x, preferred_element_type=F32).astype(BF16)
    pg[...] = jnp.dot(p, g, preferred_element_type=F32).astype(BF16)
    after = (source_row < source_col).astype(F32).astype(BF16)
    start_col = jnp.dot(after, flags, preferred_element_type=F32)
    start_col = start_col[:, lane : lane + 1].astype(jnp.int32) + rank_col[:, 0:1]
    place_col = jnp.where(flags[:, lane : lane + 1].astype(F32) > 0.5, start_col, CAP)
    pt[...] = (iota((ROWS, CAP), 1) == place_col).astype(F32).astype(BF16)


def fetch_kernel(out, pt, back):
    shrink = spread((PADDED, D), 0)
    compact = jnp.dot(out[...], shrink, preferred_element_type=F32).astype(BF16)
    rows = jnp.dot(pt[...], compact, preferred_element_type=F32).astype(BF16)
    back[...] = rows.reshape(PEERS, 2 * SLOT, D)


def mix_kernel(zl_ref, own_meta, other_meta, back, own, other):
    zl = zl_ref[0]
    rows = back[...].reshape(ROWS, D)
    q = iota((TOK, ROWS), 1)
    expert = expert_of(q, zl)
    inner = q - (q // (2 * SLOT)) * (2 * SLOT)
    block = inner // SLOT
    rank_of_slot = (inner - block * SLOT).astype(F32)
    earlier = (iota((TOK, TOK), 1) < iota((TOK, TOK), 0)).astype(F32).astype(BF16)
    for b, (meta, to) in enumerate(((own_meta, own), (other_meta, other))):
        ids = meta[:, 0:TOP].astype(jnp.int32)
        named = jnp.zeros((TOK, ROWS), F32)
        weight = jnp.zeros((TOK, ROWS), F32)
        for k in range(TOP):
            hit = ids[:, k : k + 1] == expert
            named = jnp.where(hit, 1.0, named)
            weight = jnp.where(hit, meta[:, TOP + k : TOP + k + 1], weight)
        rank = jnp.dot(earlier, named.astype(BF16), preferred_element_type=F32)
        mask = (named > 0.5) & (rank == rank_of_slot) & (block == b)
        left = jnp.where(mask, weight, 0.0)
        total = jnp.zeros((TOK, D), F32)
        for _ in range(3):
            part = left.astype(BF16)
            left = left - part.astype(F32)
            total = total + jnp.dot(part, rows, preferred_element_type=F32)
        to[...] = total.astype(to.dtype)


def call(kernel, outs, *args, scalars=1, flops=0):
    specs = [pl.BlockSpec(memory_space=pltpu.SMEM)] * scalars
    specs += [pl.BlockSpec(memory_space=pltpu.VMEM)] * (len(args) - scalars)
    shapes = [jax.ShapeDtypeStruct(s, t) for s, t in outs]
    return pl.pallas_call(
        kernel,
        out_shape=shapes,
        in_specs=specs,
        out_specs=[pl.BlockSpec(memory_space=pltpu.VMEM)] * len(shapes),
        cost_estimate=pl.CostEstimate(flops=flops, transcendentals=0, bytes_accessed=8 << 20),
        compiler_params=pltpu.CompilerParams(vmem_limit_bytes=56 << 20),
        name=kernel.__name__,
    )(*args)


def gathered(shard):
    half = WIDE // 2
    low = send(shard, UP)
    high = send(shard, DOWN)
    far = jnp.concatenate([send(low[:half], UP), send(high[half:], DOWN)], axis=0)
    mine = jnp.stack([shard, high, far, low])
    theirs = send(mine, CORES)
    z = lax.axis_index("dp") // 2
    c = lax.axis_index("dp") % 2
    mine = jnp.roll(mine, z, axis=0)
    theirs = jnp.roll(theirs, z, axis=0)
    pair = jnp.where(c == 0, jnp.stack([mine, theirs], axis=1), jnp.stack([theirs, mine], axis=1))
    return pair.reshape(PADDED, FH)


def summed(grad):
    grad = grad.reshape(4, 2, WIDE, FH)
    z = lax.axis_index("dp") // 2
    c = lax.axis_index("dp") % 2
    half = WIDE // 2
    away = lax.dynamic_index_in_dim(grad, 1 - c, 1, keepdims=False)
    keep = lax.dynamic_index_in_dim(grad, c, 1, keepdims=False)
    away = send(away, CORES)

    def part(k):
        at = (z + k) % 4
        a = lax.dynamic_index_in_dim(keep, at, 0, keepdims=False)
        b = lax.dynamic_index_in_dim(away, at, 0, keepdims=False)
        return a.astype(F32) + b.astype(F32)

    far = part(2).astype(BF16)
    first = send(far[:half], UP)
    second = send(far[half:], DOWN)
    up = part(1)
    down = part(3)
    up = jnp.concatenate([up[:half] + first.astype(F32), up[half:]], axis=0).astype(BF16)
    down = jnp.concatenate([down[:half], down[half:] + second.astype(F32)], axis=0).astype(BF16)
    up = send(up, UP)
    down = send(down, DOWN)
    total = part(0) + up.astype(F32) + down.astype(F32)
    return total.astype(BF16)[None, :CHUNK]


def body(tokens, cotangent, expert_ids, gate_weights, w_gate, w_up, w_down):
    zl = ((lax.axis_index("expert") // 4) % 2).astype(jnp.int32).reshape(1)
    meta = jnp.concatenate([expert_ids.astype(F32), gate_weights], axis=1)
    meta_t = meta.T
    other_x = send(tokens, PAIRS)
    other_c = send(cotangent, PAIRS)
    other_t = send(meta_t, PAIRS)
    full_gate, full_up, full_down = (
        gathered(jnp.pad(w[0], ((0, WIDE - CHUNK), (0, 0)))) for w in (w_gate, w_up, w_down)
    )
    (slots,) = call(
        slots_kernel,
        [((PEERS, 4 * SLOT, PADDED), BF16)],
        zl, tokens, other_x, cotangent, other_c, meta_t, other_t,
        flops=4 << 30,
    )
    recv = lax.all_to_all(
        slots, "expert", split_axis=0, concat_axis=0, tiled=True, axis_index_groups=PLANES
    )
    px, pg, pt = call(
        pack_kernel,
        [((CAP, PADDED), BF16), ((CAP, PADDED), BF16), ((ROWS, CAP), BF16)],
        zl, recv,
        flops=3 << 30,
    )
    pre_gate = jnp.dot(px, full_gate, preferred_element_type=F32)
    pre_up = jnp.dot(px, full_up, preferred_element_type=F32)
    sig = jax.nn.sigmoid(SWISH_SLOPE * pre_gate)
    value = pre_gate * sig
    slope = sig + SWISH_SLOPE * pre_gate * sig * (1.0 - sig)
    hidden = (value * (pre_up + 1.0)).astype(BF16)
    over_rows = (((0,), (0,)), ((), ()))
    grad_down = lax.dot_general(pg, hidden, over_rows, preferred_element_type=F32).astype(BF16)
    grad_down = summed(grad_down)
    d_hidden = jnp.dot(pg, full_down, preferred_element_type=F32)
    d_gate = (d_hidden * (pre_up + 1.0) * slope).astype(BF16)
    d_up = (d_hidden * value).astype(BF16)
    grad_gate = lax.dot_general(px, d_gate, over_rows, preferred_element_type=F32).astype(BF16)
    grad_gate = summed(grad_gate)
    grad_up = lax.dot_general(px, d_up, over_rows, preferred_element_type=F32).astype(BF16)
    grad_up = summed(grad_up)
    out = lax.dot_general(
        hidden, full_down, (((1,), (1,)), ((), ())), preferred_element_type=F32
    ).astype(BF16)
    (back,) = call(fetch_kernel, [((PEERS, 2 * SLOT, D), BF16)], out, pt, scalars=0, flops=4 << 30)
    back = lax.all_to_all(
        back, "expert", split_axis=0, concat_axis=0, tiled=True, axis_index_groups=PLANES
    )
    own, other = call(
        mix_kernel,
        [((TOK, D), F32), ((TOK, D), BF16)],
        zl, meta, other_t.T, back,
        flops=2 << 30,
    )
    mixed = (own + send(other, PAIRS).astype(F32)).astype(BF16)
    return mixed, grad_gate, grad_up, grad_down


def solution(mesh):
    rows = P(("expert", "dp"), None)
    weights = P("expert", "dp", None)
    return jax.shard_map(
        body,
        mesh=mesh,
        in_specs=(rows, rows, rows, rows, weights, weights, weights),
        out_specs=(rows, weights, weights, weights),
        check_vma=False,
    )
```

```python
import jax
import jax.numpy as jnp
from jax import lax
from jax.experimental import pallas as pl
from jax.experimental.pallas import tpu as pltpu
from jax.sharding import PartitionSpec as P


D = 1440
FH = 1440
CHUNK = 180
WIDE = 192
PADDED = 8 * WIDE
TOP = 4
TOK = 128
CAP = 512
SLOT = 24
PEERS = 16
ROWS = PEERS * 2 * SLOT
SWISH_SLOPE = 1.702
AXES = ("expert", "dp")
F32 = jnp.float32
BF16 = jnp.bfloat16


def device(e, d):
    return e * 8 + d


def zring(step):
    return [
        (device(e, z * 2 + c), device(e, ((z + step) % 4) * 2 + c))
        for e in range(32)
        for z in range(4)
        for c in range(2)
    ]


UP = zring(1)
DOWN = zring(-1)
CORES = [(device(e, d), device(e, d ^ 1)) for e in range(32) for d in range(8)]
PAIRS = [(device(e, d), device(e ^ 4, d)) for e in range(32) for d in range(8)]
PLANES = [[x * 8 + zl * 4 + y for x in range(4) for y in range(4)] for zl in range(2)]


def send(value, perm):
    return lax.ppermute(value, AXES, perm)


def iota(shape, dim):
    return lax.broadcasted_iota(jnp.int32, shape, dim)


def spread(shape, wide_dim, place):
    z, c = place[1], place[2]
    narrow = iota(shape, 1 - wide_dim)
    line = iota((1, PADDED) if wide_dim else (PADDED, 1), wide_dim)
    block = line // WIDE
    within = line - block * WIDE
    side = block // 4
    at = z + block - side * 4
    at = jnp.where(at >= 4, at - 4, at)
    origin = (at * 2 + jnp.where(side == 0, c, 1 - c)) * CHUNK + within
    origin = jnp.where(within < CHUNK, origin, -1)
    return (narrow == origin).astype(F32).astype(BF16)


def expert_of(q, zl):
    peer = q // (2 * SLOT)
    return (peer // 4) * 8 + zl * 4 + (peer - (peer // 4) * 4)


def slots_kernel(zl_ref, own_x, other_x, own_c, other_c, own_meta, other_meta, out):
    zl = zl_ref[0]
    grow = spread((D, PADDED), 1, zl_ref)
    used = jnp.zeros((1, PADDED), F32) + (iota((1, PADDED), 1) == CHUNK).astype(F32)
    x = jnp.concatenate([own_x[...], other_x[...]], axis=0)
    c = jnp.concatenate([own_c[...], other_c[...]], axis=0)
    xe = (jnp.dot(x, grow, preferred_element_type=F32) + used).astype(BF16)
    ce = jnp.dot(c, grow, preferred_element_type=F32).astype(BF16)
    q = iota((ROWS, TOK), 0)
    expert = expert_of(q, zl)
    inner = q - (q // (2 * SLOT)) * (2 * SLOT)
    block = inner // SLOT
    rank_of_slot = (inner - block * SLOT).astype(F32)
    earlier = (iota((TOK, TOK), 0) < iota((TOK, TOK), 1)).astype(F32).astype(BF16)
    masks = []
    gate = jnp.zeros((ROWS, 1), F32)
    for b, meta in enumerate((own_meta, other_meta)):
        ids = meta[0:TOP, :].astype(jnp.int32)
        named = jnp.zeros((ROWS, TOK), F32)
        weight = jnp.zeros((ROWS, TOK), F32)
        for k in range(TOP):
            hit = ids[k : k + 1, :] == expert
            named = jnp.where(hit, 1.0, named)
            weight = jnp.where(hit, meta[TOP + k : TOP + k + 1, :], weight)
        rank = jnp.dot(named.astype(BF16), earlier, preferred_element_type=F32)
        mask = (named > 0.5) & (rank == rank_of_slot) & (block == b)
        masks.append(mask.astype(F32).astype(BF16))
        gate = gate + jnp.sum(jnp.where(mask, weight, 0.0), axis=1, keepdims=True)
    m = jnp.concatenate(masks, axis=1)
    sx = jnp.dot(m, xe, preferred_element_type=F32).astype(BF16)
    sc = (jnp.dot(m, ce, preferred_element_type=F32) * gate).astype(BF16)
    out[:, 0 : 2 * SLOT, :] = sx.reshape(PEERS, 2 * SLOT, PADDED)
    out[:, 2 * SLOT : 4 * SLOT, :] = sc.reshape(PEERS, 2 * SLOT, PADDED)


def source_of(q, zl):
    peer = q // (2 * SLOT)
    inner = q - peer * (2 * SLOT)
    block = inner // SLOT
    plane = jnp.where(block == 0, zl, 1 - zl)
    return (peer // 4) * 8 + plane * 4 + (peer - (peer // 4) * 4), inner - block * SLOT


def pack_kernel(zl_ref, recv, px, px_t, pg, pg_t, pt):
    zl = zl_ref[0]
    x = recv[:, 0 : 2 * SLOT, :].reshape(ROWS, PADDED)
    g = recv[:, 2 * SLOT : 4 * SLOT, :].reshape(ROWS, PADDED)
    flags = x[:, 128:256]
    lane = CHUNK - 128
    source_row, rank_row = source_of(iota((ROWS, ROWS), 1), zl)
    source_col, rank_col = source_of(iota((ROWS, ROWS), 0), zl)
    before = (source_col < source_row).astype(F32).astype(BF16)
    same = (iota((ROWS, ROWS), 0) == iota((ROWS, ROWS), 1)).astype(F32).astype(BF16)
    contract = (((0,), (0,)), ((), ()))
    start_row = lax.dot_general(flags, before, contract, preferred_element_type=F32)
    used_row = lax.dot_general(flags, same, contract, preferred_element_type=F32)
    start_row = start_row[lane : lane + 1, :].astype(jnp.int32) + rank_row[0:1, :]
    place_row = jnp.where(used_row[lane : lane + 1, :] > 0.5, start_row, CAP)
    p = (iota((CAP, ROWS), 0) == place_row).astype(F32).astype(BF16)
    for rows, straight, turned in ((x, px, px_t), (g, pg, pg_t)):
        packed = jnp.dot(p, rows, preferred_element_type=F32).astype(BF16)
        straight[...] = packed
        turned[...] = packed.T
    after = (source_row < source_col).astype(F32).astype(BF16)
    start_col = jnp.dot(after, flags, preferred_element_type=F32)
    start_col = start_col[:, lane : lane + 1].astype(jnp.int32) + rank_col[:, 0:1]
    place_col = jnp.where(flags[:, lane : lane + 1].astype(F32) > 0.5, start_col, CAP)
    pt[...] = (iota((ROWS, CAP), 1) == place_col).astype(F32).astype(BF16)


COLS = 256
BLOCKS = -(-FH // COLS)


def assemble(pieces, full):
    half = WIDE // 2
    starts = [(0, WIDE), (WIDE, WIDE), (2 * WIDE, half), (2 * WIDE + half, half), (3 * WIDE, WIDE)]
    for i, piece in enumerate(pieces):
        at, size = starts[i % 5]
        at += (i // 5) * 4 * WIDE
        full[:, at : at + size, :] = piece[...]


def split(grad, keep, away):
    grad = grad.astype(BF16).reshape(2, 4, WIDE, COLS)
    keep[...] = grad[0]
    away[...] = grad[1]


def up_kernel(*refs):
    pieces, (px, pg_t, hidden, fg, fu, keep, away, full) = refs[:10], refs[10:]
    assemble(pieces, full)
    g = jnp.dot(px[...], full[0], preferred_element_type=F32)
    u = jnp.dot(px[...], full[1], preferred_element_type=F32) + 1.0
    sig = jax.nn.sigmoid(SWISH_SLOPE * g)
    value = g * sig
    hid = (value * u).astype(BF16)
    hidden[...] = hid
    fg[...] = u * (sig + SWISH_SLOPE * value * (1.0 - sig))
    fu[...] = value
    split(jnp.dot(pg_t[...], hid, preferred_element_type=F32), keep, away)


def down_kernel(*refs):
    pieces, (pg, px_t, fg, fu, keep_g, away_g, keep_u, away_u, full) = refs[:10], refs[10:]
    assemble(pieces, full)
    d = jnp.dot(pg[...], full[0], preferred_element_type=F32)
    dg = (d * fg[...]).astype(BF16)
    du = (d * fu[...]).astype(BF16)
    split(jnp.dot(px_t[...], dg, preferred_element_type=F32), keep_g, away_g)
    split(jnp.dot(px_t[...], du, preferred_element_type=F32), keep_u, away_u)


def fetch_kernel(*refs):
    pieces, (place, hidden, pt, back, full, total) = refs[:10], refs[10:]
    n = pl.program_id(0)
    assemble(pieces, full)

    @pl.when(n == 0)
    def _():
        total[...] = jnp.zeros_like(total)

    inside = iota((1, COLS), 1) < FH - n * COLS
    hid = jnp.where(inside, hidden[...].astype(F32), 0.0).astype(BF16)
    mat = jnp.where(inside, full[0].astype(F32), 0.0).astype(BF16)
    total[...] += lax.dot_general(hid, mat, (((1,), (1,)), ((), ())), preferred_element_type=F32)

    @pl.when(n == BLOCKS - 1)
    def _():
        shrink = spread((PADDED, D), 0, place)
        out = total[...].astype(BF16)
        compact = jnp.dot(out, shrink, preferred_element_type=F32).astype(BF16)
        rows = jnp.dot(pt[...], compact, preferred_element_type=F32).astype(BF16)
        back[...] = rows.reshape(PEERS, 2 * SLOT, D)


def mix_kernel(zl_ref, own_meta, other_meta, back, own, other):
    zl = zl_ref[0]
    rows = back[...].reshape(ROWS, D)
    q = iota((TOK, ROWS), 1)
    expert = expert_of(q, zl)
    inner = q - (q // (2 * SLOT)) * (2 * SLOT)
    block = inner // SLOT
    rank_of_slot = (inner - block * SLOT).astype(F32)
    earlier = (iota((TOK, TOK), 1) < iota((TOK, TOK), 0)).astype(F32).astype(BF16)
    for b, (meta, to) in enumerate(((own_meta, own), (other_meta, other))):
        ids = meta[:, 0:TOP].astype(jnp.int32)
        named = jnp.zeros((TOK, ROWS), F32)
        weight = jnp.zeros((TOK, ROWS), F32)
        for k in range(TOP):
            hit = ids[:, k : k + 1] == expert
            named = jnp.where(hit, 1.0, named)
            weight = jnp.where(hit, meta[:, TOP + k : TOP + k + 1], weight)
        rank = jnp.dot(earlier, named.astype(BF16), preferred_element_type=F32)
        mask = (named > 0.5) & (rank == rank_of_slot) & (block == b)
        left = jnp.where(mask, weight, 0.0)
        total = jnp.zeros((TOK, D), F32)
        for _ in range(3):
            part = left.astype(BF16)
            left = left - part.astype(F32)
            total = total + jnp.dot(part, rows, preferred_element_type=F32)
        to[...] = total.astype(to.dtype)


SMEM = pltpu.SMEM
VMEM = pltpu.VMEM


def whole(a):
    return pl.BlockSpec(a.shape, lambda n: (0,) * len(a.shape))


def by_columns(a):
    lead = len(a.shape) - 1
    return pl.BlockSpec((*a.shape[:-1], COLS), lambda n: (0,) * lead + (n,))


def scalars(a):
    return pl.BlockSpec(memory_space=SMEM)


def vector(a):
    return pl.BlockSpec(memory_space=VMEM)


def call(kernel, outs, *groups, flops=0, scratch=(), grid=None, out_spec=vector):
    args = [a for _, group in groups for a in group]
    shapes = [jax.ShapeDtypeStruct(s, t) for s, t in outs]
    return pl.pallas_call(
        kernel,
        out_shape=shapes,
        in_specs=[spec(a) for spec, group in groups for a in group],
        out_specs=[out_spec(a) for a in shapes],
        scratch_shapes=list(scratch),
        **({"grid": grid} if grid else {}),
        cost_estimate=pl.CostEstimate(flops=flops, transcendentals=0, bytes_accessed=8 << 20),
        compiler_params=pltpu.CompilerParams(vmem_limit_bytes=56 << 20),
    )(*args)


def gathered(shard):
    half = WIDE // 2
    low = send(shard, UP)
    high = send(shard, DOWN)
    near, far = send(low[:, :half], UP), send(high[:, half:], DOWN)
    mine = [shard, high, near, far, low]
    return mine + [send(piece, CORES) for piece in mine]


def summed(keep, away):
    half = WIDE // 2
    away = send(away, CORES)

    def part(k, rows):
        return keep[k, rows].astype(F32) + away[k, rows].astype(F32)

    low, high = slice(0, half), slice(half, WIDE)
    first = send(part(2, low).astype(BF16), UP)
    second = send(part(2, high).astype(BF16), DOWN)
    up = jnp.concatenate([part(1, low) + first.astype(F32), part(1, high)], axis=0)
    down = jnp.concatenate([part(3, low), part(3, high) + second.astype(F32)], axis=0)
    up = send(up.astype(BF16), UP)
    down = send(down.astype(BF16), DOWN)
    total = part(0, slice(0, WIDE)) + up.astype(F32) + down.astype(F32)
    return total.astype(BF16)[None, :CHUNK]


def step(tokens, cotangent, expert_ids, gate_weights, w_gate, w_up, w_down):
    e, d = lax.axis_index("expert"), lax.axis_index("dp")
    place = jnp.stack([(e >> 2) & 1, d >> 1, d & 1]).astype(jnp.int32)
    meta = jnp.concatenate([expert_ids.astype(F32), gate_weights], axis=1)
    meta_t = meta.T
    other_t = send(meta_t, PAIRS)
    other_x = send(tokens, PAIRS)
    other_c = send(cotangent, PAIRS)
    tail = ((0, 0), (0, WIDE - CHUNK), (0, 0))
    gate_up = gathered(jnp.pad(jnp.concatenate([w_gate, w_up], axis=0), tail))
    downs = gathered(jnp.pad(w_down, tail))
    (slots,) = call(
        slots_kernel,
        [((PEERS, 4 * SLOT, PADDED), BF16)],
        (scalars, [place]),
        (vector, [tokens, other_x, cotangent, other_c, meta_t, other_t]),
        flops=4 << 30,
    )
    recv = lax.all_to_all(
        slots, "expert", split_axis=0, concat_axis=0, tiled=True, axis_index_groups=PLANES
    )
    straight, turned = ((CAP, PADDED), BF16), ((PADDED, CAP), BF16)
    px, px_t, pg, pg_t, pt = call(
        pack_kernel,
        [straight, turned, straight, turned, ((ROWS, CAP), BF16)],
        (scalars, [place]),
        (vector, [recv]),
        flops=3 << 30,
    )
    part = ((4, WIDE, FH), BF16)
    hidden, fg, fu, keep, away = call(
        up_kernel,
        [((CAP, FH), BF16), ((CAP, FH), F32), ((CAP, FH), F32), part, part],
        (by_columns, gate_up),
        (whole, [px, pg_t]),
        flops=7 << 30,
        scratch=[VMEM((2, PADDED, COLS), BF16)],
        grid=(BLOCKS,),
        out_spec=by_columns,
    )
    grad_down = summed(keep, away)
    keep_g, away_g, keep_u, away_u = call(
        down_kernel,
        [part, part, part, part],
        (by_columns, downs),
        (whole, [pg, px_t]),
        (by_columns, [fg, fu]),
        flops=7 << 30,
        scratch=[VMEM((1, PADDED, COLS), BF16)],
        grid=(BLOCKS,),
        out_spec=by_columns,
    )
    grad_gate = summed(keep_g, away_g)
    grad_up = summed(keep_u, away_u)
    (back,) = call(
        fetch_kernel,
        [((PEERS, 2 * SLOT, D), BF16)],
        (by_columns, downs),
        (scalars, [place]),
        (by_columns, [hidden]),
        (whole, [pt]),
        flops=5 << 30,
        scratch=[VMEM((1, PADDED, COLS), BF16), VMEM((CAP, PADDED), F32)],
        grid=(BLOCKS,),
        out_spec=whole,
    )
    back = lax.all_to_all(
        back, "expert", split_axis=0, concat_axis=0, tiled=True, axis_index_groups=PLANES
    )
    own, other = call(
        mix_kernel,
        [((TOK, D), F32), ((TOK, D), BF16)],
        (scalars, [place]),
        (vector, [meta, other_t.T, back]),
        flops=2 << 30,
    )
    mixed = (own + send(other, PAIRS).astype(F32)).astype(BF16)
    return mixed, grad_gate, grad_up, grad_down


def solution(mesh):
    rows = P(("expert", "dp"), None)
    weights = P("expert", "dp", None)
    return jax.shard_map(
        step,
        mesh=mesh,
        in_specs=(rows, rows, rows, rows, weights, weights, weights),
        out_specs=(rows, weights, weights, weights),
        check_vma=False,
    )
```
